32 devices in a mesh: ell: 4 (over y, x), blk: 8 (over z, core).
Axes of the slice: x: 2, y: 2, z: 4, core: 2. Of those that a mesh axis runs over, the one named last changes fastest.
Arguments:
- wigner: bfloat16 [8, 17, 2101248], P(None, None, ('ell', 'blk')), may hold values from -6 to 6
- sky_alm: float32 [2, 2101248], P(None, ('ell', 'blk')), may hold values from -0.03125 to 0.03125
- beam_blm: float32 [2, 17, 2048], replicated, may hold values from -4.25 to 4.25
- slot_col: int32 [2101248], P(('ell', 'blk')), may hold values from -1 to 255, as said below
- slot_ell: int32 [2101248], P(('ell', 'blk')), may hold values from 0 to 2047, as said below
- order_of_column: int32 [2048], replicated, may hold values from 0 to 2047, as said below
Outputs:
- conv_cube: float32 [8, 32, 4096], P('ell', 'blk')
The draws below stay inside these ranges and needn't reach their ends.
Inputs may be any that keep to these rules, and one draw needn't show every extreme that they name: `slot_col`: slot block b (slots b * 65664 to b * 65664 + 65663) belongs to ell index b // 8 and blk index b % 8; at most 65568 slots of a block are live, and some blocks have exactly that many. `slot_ell`: every pair (l, m) with m <= l < 2048 stands in exactly one live slot; within a blk group, higher ell indices hold degrees no lower than those of lower ell indices. `order_of_column`: A permutation of 0 to 2047; every blk group's orders hold the same number of pairs.
All inputs are finite; a program needn't handle non-finite values.
Results may differ from the reference program's by a relative error of at most 0.0029.
Values sent between devices are 32-bit elements; how exact they have to be, the bound alone decides.
No kernel may reach another device: no remote copies, remote signals or barrier semaphores. Data moves between devices by JAX's collectives and lax.ppermute only.
A program may use at most 256 MiB of HBM per device.

```python
import math
import jax
import jax.numpy as jnp
from jax import lax

L = 2048
K = 17
NPSI = 32
THETA = 8
NPHI = 4096
M_DEV = 256
LIVE_MOST = 65568
SLOT_DEV = 65664
SLOTS = 2101248
N_ELL = 4
N_BLK = 8


def pair_tables(key):
    half = L // 2
    fold = L // (2 * N_BLK)
    blocks = N_ELL * N_BLK
    cols = L // N_BLK
    order = jax.random.permutation(jax.random.fold_in(key, 101), half)
    lower = order.reshape(N_BLK, fold)
    grouped = jnp.concatenate([lower, L - 1 - lower], axis=1).astype(jnp.int32)
    col_keys = jax.random.split(jax.random.fold_in(key, 102), N_BLK)
    col_perm = jax.vmap(lambda inner_key: jax.random.permutation(inner_key, cols))(col_keys)
    order_table = jnp.take_along_axis(grouped, col_perm.astype(jnp.int32), axis=1)
    degrees = jnp.arange(L, dtype=jnp.int32)
    valid = order_table[:, None, :] <= degrees[None, :, None]
    flat_valid = valid.reshape(N_BLK, L * cols)
    position = jnp.cumsum(flat_valid.astype(jnp.int32), axis=1) - 1
    ell_index = position // LIVE_MOST
    offset = jnp.clip(position % LIVE_MOST, 0, SLOT_DEV - 1)
    group_index = jnp.arange(N_BLK, dtype=jnp.int32)[:, None]
    block = jnp.clip(ell_index * N_BLK + group_index, 0, blocks - 1)
    shuffle_keys = jax.random.split(jax.random.fold_in(key, 103), blocks)
    shuffles = jax.vmap(lambda inner_key: jax.random.permutation(inner_key, SLOT_DEV))(shuffle_keys).astype(jnp.int32)
    slot = block * SLOT_DEV + shuffles[block, offset]
    target = jnp.where(flat_valid, slot, blocks * SLOT_DEV).reshape(-1)
    col_values = jnp.broadcast_to(jnp.arange(cols, dtype=jnp.int32)[None, None, :], (N_BLK, L, cols)).reshape(-1)
    ell_values = jnp.broadcast_to(degrees[None, :, None], (N_BLK, L, cols)).reshape(-1)
    slot_col = jnp.full((blocks * SLOT_DEV,), -1, jnp.int32).at[target].set(col_values, mode='drop')
    slot_ell = jnp.zeros((blocks * SLOT_DEV,), jnp.int32).at[target].set(ell_values, mode='drop')
    return (order_table.reshape(L), slot_col, slot_ell)


def draw_order_of_column(key, part):
    return pair_tables(key)[0]


def draw_slot_col(key, part):
    return pair_tables(key)[1]


def draw_slot_ell(key, part):
    return pair_tables(key)[2]


def draw_beam_blm(key, part):
    degrees = jnp.arange(L, dtype=jnp.float32)
    scale = (2.0 * (degrees + 1.0)) ** (-0.5)
    base = jnp.clip(jax.random.normal(key, (2, K, L), jnp.float32), -6.0, 6.0)
    return (base * scale[None, None, :]).astype(jnp.float32)


def level_of(key, shape, pieces, low, top_value):
    def one(dim, blocks):
        draws = jax.random.uniform(jax.random.fold_in(jax.random.fold_in(key, 6), dim), (blocks,), jnp.float32, low / len(pieces), top_value / len(pieces))
        return jnp.repeat(jnp.exp(draws), shape[dim] // blocks).reshape((-1,) + (1,) * (len(shape) - dim - 1))

    gain = one(*pieces[0])
    for cut in pieces[1:]:
        gain = gain * one(*cut)
    return gain


def scatter_about(rng, shape, deviation, reach, shards=(), held_as=jnp.bfloat16):
    array = jax.random.normal(rng, shape, jnp.float32) * deviation
    if len(shards) > 0:
        array = level_of(rng, shape, shards, -0.22, 0.18) * array
    return jnp.clip(array, min=-reach, max=reach).astype(held_as)


def setup_inputs(seed: int = 0) -> dict:
    key_of = jax.random.split(jax.random.key(seed), 7)
    wigner = scatter_about(key_of[0], (THETA, K, SLOTS), 1.0, 6.0, ((2, 32),))
    sky_alm = scatter_about(key_of[1], (2, SLOTS), (L * K) ** -0.5, 0.03125, ((1, 32),), jnp.float32)
    beam_blm = draw_beam_blm(jax.random.fold_in(key_of[6], 71), 0)
    slot_col = draw_slot_col(jax.random.fold_in(key_of[6], 71), 0)
    slot_ell = draw_slot_ell(jax.random.fold_in(key_of[6], 71), 0)
    order_of_column = draw_order_of_column(jax.random.fold_in(key_of[6], 71), 0)
    return dict(wigner=wigner, sky_alm=sky_alm, beam_blm=beam_blm, slot_col=slot_col, slot_ell=slot_ell, order_of_column=order_of_column)


def phase_table(rows, cols, period):
    product = (jnp.arange(rows, dtype=jnp.int32)[:, None] * jnp.arange(cols, dtype=jnp.int32)[None, :]) % period
    angle = product.astype(jnp.float32) * (2.0 * math.pi / period)
    return jnp.cos(angle), jnp.sin(angle)


def psi_table(order_count, samples):
    cosines, sine_terms = phase_table(order_count, samples, samples)
    real_row = jnp.stack([cosines, sine_terms], axis=1)
    imag_row = jnp.stack([-sine_terms, cosines], axis=1)
    return jnp.stack([real_row, imag_row], axis=0)


def reference(wigner, sky_alm, beam_blm, slot_col, slot_ell, order_of_column):
    block_count = SLOTS // SLOT_DEV

    def accumulate(running, block_index):
        first_slot = block_index * SLOT_DEV
        wig_rows = lax.dynamic_slice_in_dim(wigner, first_slot, SLOT_DEV, 2).astype(jnp.float32)
        alm_part = lax.dynamic_slice_in_dim(sky_alm, first_slot, SLOT_DEV, 1)
        columns = lax.dynamic_slice_in_dim(slot_col, first_slot, SLOT_DEV, 0)
        degrees = lax.dynamic_slice_in_dim(slot_ell, first_slot, SLOT_DEV, 0)
        beam_slots = jnp.take(beam_blm, degrees, axis=2)
        coeffs = jnp.stack([alm_part[0] * beam_slots[0] - alm_part[1] * beam_slots[1],
                            alm_part[0] * beam_slots[1] + alm_part[1] * beam_slots[0]])
        values = (wig_rows[:, None] * coeffs[None]).astype(jnp.bfloat16)
        values = lax.optimization_barrier(values).astype(jnp.float32)
        group = (block_index % N_BLK).astype(jnp.int32)
        global_col = group * M_DEV + jnp.maximum(columns, 0)
        orders = jnp.where(columns >= 0, jnp.take(order_of_column, global_col), L).astype(jnp.int32)
        flat = values.reshape(THETA * 2 * K, SLOT_DEV).T
        return running + jax.ops.segment_sum(flat, orders, num_segments=L + 1)[:L], None

    totals, _ = lax.scan(accumulate, jnp.zeros((L, THETA * 2 * K), jnp.float32),
                         jnp.arange(block_count, dtype=jnp.int32))
    harmonic = totals.T.reshape(THETA, 2, K, L)
    psi_field = jnp.einsum("trkc,rksp->tspc", harmonic, psi_table(K, NPSI), precision=lax.Precision.HIGHEST)
    complex_field = psi_field[:, 0] + 1j * psi_field[:, 1]
    padded = jnp.pad(complex_field, ((0, 0), (0, 0), (0, NPHI - L)))
    return (jnp.real(jnp.fft.ifft(padded, axis=-1)) * NPHI).astype(jnp.float32)
```

```python
import functools
import math

import jax
import jax.numpy as jnp
from jax import lax
from jax.experimental import pallas as pl
from jax.experimental.pallas import tpu as pltpu
from jax.sharding import PartitionSpec as P

NPSI = 32
LANES = 128
TILE = 256
F32 = jnp.float32
BF16 = jnp.bfloat16


def phase_table(rows, cols, period):
    product = (
        jnp.arange(rows, dtype=jnp.int32)[:, None]
        * jnp.arange(cols, dtype=jnp.int32)[None, :]
        % period
    )
    angle = product.astype(jnp.float32) * (2.0 * math.pi / period)
    return (jnp.cos(angle), jnp.sin(angle))


def psi_table(order_count, samples):
    cosines, sine_terms = phase_table(order_count, samples, samples)
    real_row = jnp.stack([cosines, sine_terms], axis=1)
    imag_row = jnp.stack([-sine_terms, cosines], axis=1)
    return jnp.stack([real_row, imag_row], axis=0)


def to_psi(harmonic, table):
    return jnp.einsum("trkc,rksp->tspc", harmonic, table, precision=lax.Precision.HIGHEST)


def to_phi(fields, order_of_column):
    cycles = fields.shape[0]
    samples = fields.shape[2]
    degrees = fields.shape[3]
    period = 2 * degrees
    inner = 2 ** ((period.bit_length() - 1) // 2)
    outer = period // inner
    highest = lax.Precision.HIGHEST
    high_part = order_of_column // inner
    low_part = order_of_column % inner
    turns = high_part[:, None] * jnp.arange(outer, dtype=jnp.int32)[None, :] % outer
    angle = turns.astype(jnp.float32) * (2.0 * math.pi / outer)
    cos_first = jnp.cos(angle)
    sin_first = jnp.sin(angle)
    select = (low_part[:, None] == jnp.arange(inner, dtype=jnp.int32)[None, :]).astype(jnp.float32)
    real_in = fields[:, 0]
    imag_in = fields[:, 1]
    weighted_re = real_in[..., None] * cos_first - imag_in[..., None] * sin_first
    weighted_im = real_in[..., None] * sin_first + imag_in[..., None] * cos_first
    first_re = jnp.einsum("tpcj,cv->tpvj", weighted_re, select, precision=highest)
    first_im = jnp.einsum("tpcj,cv->tpvj", weighted_im, select, precision=highest)
    cos_twist, sin_twist = phase_table(inner, outer, period)
    twist_re = first_re * cos_twist - first_im * sin_twist
    twist_im = first_re * sin_twist + first_im * cos_twist
    cos_last, sin_last = phase_table(inner, inner, inner)
    result = jnp.einsum("tpvj,vw->tpwj", twist_re, cos_last, precision=highest) - jnp.einsum(
        "tpvj,vw->tpwj", twist_im, sin_last, precision=highest
    )
    return result.reshape(cycles, samples, period)


def sums_kernel(
    shape, base_ref, table_ref, *refs
):
    (cycles, orders, cols, spans, chunk, main_steps) = shape
    streams, (out_ref, values_ref) = refs[:-2], refs[-2:]
    step = pl.program_id(0)
    full = orders // 16 * 16
    pair = 2 * full

    def one_hot(row, count):
        rows = lax.broadcasted_iota(jnp.int32, (count, row.shape[1]), 0).astype(F32).astype(BF16)
        match = row.astype(F32).astype(BF16) == rows
        return jnp.where(match, jnp.ones_like(rows), jnp.zeros_like(rows))

    def add_chunk(w_ref, sky_ref, col_ref, ell_ref, offset, width):
        where = pl.ds(offset, width)
        index = ell_ref[:, where] - base_ref[0]
        span = lax.shift_right_arithmetic(index, 8)
        hot_ell = one_hot(lax.bitwise_and(index, TILE - 1), TILE)
        picked = jnp.dot(table_ref[0], hot_ell, preferred_element_type=F32) + jnp.dot(
            table_ref[1], hot_ell, preferred_element_type=F32
        )
        beam_re = picked[0:full]
        beam_im = picked[full:pair]
        for j in range(1, spans):
            here = span == j
            beam_re = jnp.where(here, picked[j * pair : j * pair + full], beam_re)
            beam_im = jnp.where(here, picked[j * pair + full : (j + 1) * pair], beam_im)
        sky_re = sky_ref[0:1, where]
        sky_im = sky_ref[1:2, where]
        coef_re = sky_re * beam_re - sky_im * beam_im
        coef_im = sky_re * beam_im + sky_im * beam_re
        rows8 = lax.broadcasted_iota(jnp.int32, (8, width), 0) == span
        for k in range(orders):
            if k < full:
                row_re = coef_re[k : k + 1]
                row_im = coef_im[k : k + 1]
            else:
                at = spans * pair + (k - full) * 16
                last_re = jnp.sum(jnp.where(rows8, picked[at : at + 8], 0.0), axis=0, keepdims=True)
                last_im = jnp.sum(
                    jnp.where(rows8, picked[at + 8 : at + 16], 0.0), axis=0, keepdims=True
                )
                row_re = sky_re * last_re - sky_im * last_im
                row_im = sky_re * last_im + sky_im * last_re
            w = w_ref[k, :, where].astype(F32)
            both = jnp.concatenate([w * row_re, w * row_im], axis=0).astype(BF16)
            values_ref[k * 2 * cycles : (k + 1) * 2 * cycles, 0:width] = both
        hot_col = one_hot(col_ref[:, where], cols)
        out_ref[...] += lax.dot_general(
            values_ref[:, 0:width],
            hot_col,
            (((1,), (1,)), ((), ())),
            preferred_element_type=F32,
        )

    @pl.when(step == 0)
    def _():
        out_ref[...] = jnp.zeros_like(out_ref)

    main = streams[:4]
    block = main[0].shape[2]

    def body(i, carry):
        add_chunk(*main, pl.multiple_of(i * chunk, chunk), chunk)
        return carry

    lax.fori_loop(0, block // chunk, body, 0)

    if len(streams) > 4:

        @pl.when(step == main_steps - 1)
        def _():
            add_chunk(*streams[4:], 0, streams[4].shape[2])


def column_sums(wigner, sky_alm, table, base, slot_col, slot_ell, cols, spans):
    orders, cycles, slots = wigner.shape
    block = 4096
    chunk = 512
    steps = slots // block
    tail = slots - steps * block
    rows = 2 * orders * cycles

    def specs(width, at):
        return [
            pl.BlockSpec((orders, cycles, width), lambda i, b: (0, 0, at(i))),
            pl.BlockSpec((2, width), lambda i, b: (0, at(i))),
            pl.BlockSpec((1, width), lambda i, b: (0, at(i))),
            pl.BlockSpec((1, width), lambda i, b: (0, at(i))),
        ]

    arrays = [wigner, sky_alm, slot_col, slot_ell]
    in_specs = [pl.BlockSpec(table.shape, lambda i, b: (0, 0, 0))] + specs(block, lambda i: i)
    operands = [table] + arrays
    if tail:
        at = slots // tail - 1
        in_specs += specs(tail, lambda i: at)
        operands += arrays
    return pl.pallas_call(
        functools.partial(sums_kernel, (cycles, orders, cols, spans, chunk, steps)),
        grid_spec=pltpu.PrefetchScalarGridSpec(
            num_scalar_prefetch=1,
            grid=(steps,),
            in_specs=in_specs,
            out_specs=pl.BlockSpec((rows, cols), lambda i, b: (0, 0)),
            scratch_shapes=[pltpu.VMEM((rows, chunk), BF16)],
        ),
        out_shape=jax.ShapeDtypeStruct((rows, cols), F32),
        compiler_params=pltpu.CompilerParams(dimension_semantics=("arbitrary",)),
        name="column_sums",
    )(base, *operands)


def beam_table(beam_blm, base, spans):
    orders = beam_blm.shape[1]
    full = orders // 16 * 16
    window = lax.dynamic_slice_in_dim(beam_blm, base, spans * TILE, axis=2)
    window = window.reshape(2, orders, spans, TILE)
    head = window[:, :full].transpose(2, 0, 1, 3).reshape(spans * 2 * full, TILE)
    rest = window[:, full:].transpose(1, 0, 2, 3)
    rest = jnp.pad(rest, ((0, 0), (0, 0), (0, 8 - spans), (0, 0)))
    rows = jnp.concatenate([head, rest.reshape(-1, TILE)], axis=0)
    upper = lax.reduce_precision(rows, exponent_bits=8, mantissa_bits=7)
    return jnp.stack([upper.astype(BF16), (rows - upper).astype(BF16)])


def degree_width(degrees, ell_count, blk_count, cols):
    live = degrees * (degrees + 1) // 2 // (ell_count * blk_count)
    width = degrees - (ell_count - 1) * live // cols
    return min(degrees, -(-width // TILE) * TILE)


def on_device(wigner, sky_alm, beam_blm, slot_col, slot_ell, order_of_column):
    cycle_total = wigner.shape[0]
    order_count = wigner.shape[1]
    slot_count = wigner.shape[2]
    ell_count = lax.axis_size("ell")
    blk_count = lax.axis_size("blk")
    col_count = order_of_column.shape[0] // blk_count
    cycle_share = cycle_total // ell_count
    degree_count = beam_blm.shape[2]
    width = degree_width(degree_count, ell_count, blk_count, col_count)
    spans = width // TILE
    lowest = jnp.min(jnp.where(slot_col >= 0, slot_ell, degree_count))
    base = jnp.minimum(lowest, degree_count - width)
    col_sums = column_sums(
        jnp.transpose(wigner, (1, 0, 2)),
        sky_alm,
        beam_table(beam_blm, base, spans),
        base.reshape(1),
        slot_col.reshape(1, slot_count),
        slot_ell.reshape(1, slot_count),
        col_count,
        spans,
    )
    parts = col_sums.reshape(order_count, 2, cycle_total, col_count).transpose(2, 1, 0, 3)
    parts = parts.reshape(ell_count, cycle_share, 2, order_count, col_count)
    summed = jnp.sum(lax.all_to_all(parts, "ell", split_axis=0, concat_axis=0, tiled=True), axis=0)
    owned = to_psi(summed, psi_table(order_count, NPSI))
    return to_phi(
        lax.all_to_all(owned, "blk", split_axis=2, concat_axis=3, tiled=True), order_of_column
    )


def solution(mesh):
    return jax.shard_map(
        on_device,
        mesh=mesh,
        in_specs=(
            P(None, None, ("ell", "blk")),
            P(None, ("ell", "blk")),
            P(),
            P(("ell", "blk")),
            P(("ell", "blk")),
            P(),
        ),
        out_specs=P("ell", "blk", None),
        check_vma=False,
    )
```

```python
import functools
import math

import jax
import jax.numpy as jnp
import numpy as np
from jax import lax
from jax.experimental import pallas as pl
from jax.experimental.pallas import tpu as pltpu
from jax.sharding import PartitionSpec as P

NPSI = 32
LANES = 128
TILE = 256
BLOCK = 8192
F32 = jnp.float32
BF16 = jnp.bfloat16


def psi_matrix(blks, cycles, orders):
    samples = NPSI // blks
    p = np.arange(NPSI).reshape(blks, 1, 1, samples, 1, 1, 1)
    cycle = np.arange(cycles)
    part = np.arange(2)
    k = np.arange(orders).reshape(1, 1, 1, 1, 1, orders, 1)
    same = cycle.reshape(1, -1, 1, 1, 1, 1, 1) == cycle.reshape(1, 1, 1, 1, -1, 1, 1)
    out_part = part.reshape(1, 1, 2, 1, 1, 1, 1)
    in_part = part.reshape(1, 1, 1, 1, 1, 1, 2)
    angle = 2.0 * np.pi * (k * p % NPSI) / NPSI
    turned = np.where(in_part == out_part, np.cos(angle), (out_part - in_part) * np.sin(angle))
    matrix = np.where(same, turned, 0.0).astype(np.float32)
    return matrix.reshape(blks * cycles * 2 * samples, cycles * orders * 2)


def psi_kernel(matrix_ref, parts_ref, out_ref):
    total = parts_ref[0]
    for e in range(1, parts_ref.shape[0]):
        total = total + parts_ref[e]
    out_ref[...] = jnp.dot(
        matrix_ref[...], total, precision=lax.Precision.HIGHEST, preferred_element_type=F32
    )


def to_psi(parts, blks, cycles, orders):
    matrix = psi_matrix(blks, cycles, orders)
    rows, cols = matrix.shape[0], parts.shape[2]
    out = pl.pallas_call(
        psi_kernel,
        out_shape=jax.ShapeDtypeStruct((rows, cols), F32),
        compiler_params=pltpu.CompilerParams(vmem_limit_bytes=16 * 2**20),
        name="psi",
    )(jnp.asarray(matrix), parts)
    return out.reshape(blks, rows // blks, cols)


def halves(array):
    upper = lax.reduce_precision(array, exponent_bits=8, mantissa_bits=7)
    return upper.astype(BF16), (array - upper).astype(BF16)


def phi_tables(order_of_column, period):
    def waves(step, count):
        turns = jnp.arange(count, dtype=jnp.int32)[:, None] * step * order_of_column[None, :]
        angle = (turns % period).astype(F32) * (2.0 * math.pi / period)
        return jnp.cos(angle), jnp.sin(angle)

    fine_cos, fine_sin = waves(1, LANES)
    return waves(LANES, period // LANES) + halves(fine_cos) + halves(-fine_sin)


def phi_kernel(cycles, fields_ref, cos_ref, sin_ref, ch_ref, cl_ref, sh_ref, sl_ref, out_ref):
    blks, rows, cols = fields_ref.shape
    samples = rows // (2 * cycles)
    coarse = cos_ref.shape[0]

    def nt(left, right):
        return lax.dot_general(
            left, right, (((1,), (1,)), ((), ())), preferred_element_type=F32
        )

    def split(pieces):
        array = jnp.concatenate(pieces, axis=0)
        upper = array.astype(BF16)
        return upper, (array - upper.astype(F32)).astype(BF16)

    wide = None
    narrow = None
    for d in range(blks):
        where = slice(d * cols, (d + 1) * cols)
        cos, sin = cos_ref[:, where], sin_ref[:, where]
        left_re, left_im = [], []
        for t in range(cycles):
            for p in range(samples):
                at = t * 2 * samples + p
                re = fields_ref[d, at : at + 1, :]
                im = fields_ref[d, at + samples : at + samples + 1, :]
                left_re.append(re * cos - im * sin)
                left_im.append(re * sin + im * cos)
        for left, high_ref, low_ref in ((left_re, ch_ref, cl_ref), (left_im, sh_ref, sl_ref)):
            upper, lower = split(left)
            high, low = high_ref[:, where], low_ref[:, where]
            both = nt(upper, jnp.concatenate([high, low], axis=0))
            rest = nt(lower, high)
            wide = both if wide is None else wide + both
            narrow = rest if narrow is None else narrow + rest
    fine = high_ref.shape[0]
    result = wide[:, 0:fine] + (wide[:, fine:] + narrow)
    for t in range(cycles):
        for p in range(samples):
            for a in range(coarse):
                at = (t * samples + p) * coarse + a
                out_ref[t, p : p + 1, a * fine : (a + 1) * fine] = result[at : at + 1]


def to_phi(fields, tables, cycles):
    blks, rows, cols = fields.shape
    coarse, fine = tables[0].shape[0], tables[2].shape[0]
    samples = rows // (2 * cycles)
    return pl.pallas_call(
        functools.partial(phi_kernel, cycles),
        out_shape=jax.ShapeDtypeStruct((cycles, samples, coarse * fine), F32),
        compiler_params=pltpu.CompilerParams(vmem_limit_bytes=40 * 2**20),
        name="phi",
    )(fields, *tables)


def sums_kernel(shape, col_ref, ell_ref, beam_ref, *refs):
    (cycles, orders, cols, spans, block, tail, steps, shares) = shape
    streams = refs[:-6]
    out_ref, sum_ref, values_ref, table_ref, rows_ref, turn_ref = refs[-6:]
    step = pl.program_id(0)
    degrees = beam_ref.shape[2]
    full = orders // 16 * 16
    pair = 2 * full

    def lowest_degree():
        def fold(at, width, low):
            where = pl.ds(at, width)
            col = col_ref[where].reshape(1, width)
            ell = ell_ref[where].reshape(1, width).astype(F32)
            return jnp.minimum(low, jnp.min(jnp.where(col >= 0, ell, float(degrees))))

        low = float(degrees)
        low = lax.fori_loop(
            0, steps, lambda i, c: fold(pl.multiple_of(i * block, block), block, c), jnp.float32(low)
        )
        if tail:
            low = fold(steps * block, tail, low)
        return jnp.minimum(low.astype(jnp.int32), degrees - spans * TILE)

    @pl.when(step == 0)
    def _():
        sum_ref[...] = jnp.zeros_like(sum_ref)
        rows_ref[...] = jnp.zeros_like(rows_ref)
        base = lowest_degree()
        for k in range(orders):
            window = pltpu.roll(beam_ref[k], degrees - base, 1)
            for j in range(spans):
                for r in range(2):
                    row = j * pair + r * full + k
                    if k >= full:
                        row = spans * pair + (k - full) * 16 + r * 8 + j
                    rows_ref[row : row + 1, 0:TILE] = window[r : r + 1, j * TILE : (j + 1) * TILE]
        rows = rows_ref[:, 0:TILE]
        upper = rows.astype(BF16)
        table_ref[0] = upper
        table_ref[1] = (rows - upper.astype(F32)).astype(BF16)
        rows_ref[0:1, TILE:] = jnp.zeros((1, LANES), F32) + base.astype(F32)

    def one_hot(row, count):
        rows = lax.broadcasted_iota(jnp.int32, (count, row.shape[1]), 0).astype(F32).astype(BF16)
        match = row.astype(F32).astype(BF16) == rows
        return jnp.where(match, jnp.ones_like(rows), jnp.zeros_like(rows))

    def add_chunk(w_ref, sky_ref, at, width):
        where = pl.ds(at, width)
        base = rows_ref[0:1, TILE : TILE + 1].astype(jnp.int32)
        index = ell_ref[where].reshape(1, width) - base
        span = lax.shift_right_arithmetic(index, 8)
        hot_ell = one_hot(lax.bitwise_and(index, TILE - 1), TILE)
        picked = jnp.dot(table_ref[0], hot_ell, preferred_element_type=F32) + jnp.dot(
            table_ref[1], hot_ell, preferred_element_type=F32
        )
        beam_re = picked[0:full]
        beam_im = picked[full:pair]
        for j in range(1, spans):
            here = span == j
            beam_re = jnp.where(here, picked[j * pair : j * pair + full], beam_re)
            beam_im = jnp.where(here, picked[j * pair + full : (j + 1) * pair], beam_im)
        sky_re = sky_ref[0:1, :]
        sky_im = sky_ref[1:2, :]
        coef_re = sky_re * beam_re - sky_im * beam_im
        coef_im = sky_re * beam_im + sky_im * beam_re
        rows8 = lax.broadcasted_iota(jnp.int32, (8, width), 0) == span
        for k in range(orders):
            if k < full:
                row_re = coef_re[k : k + 1]
                row_im = coef_im[k : k + 1]
            else:
                top = spans * pair + (k - full) * 16
                last_re = jnp.sum(jnp.where(rows8, picked[top : top + 8], 0.0), axis=0, keepdims=True)
                last_im = jnp.sum(
                    jnp.where(rows8, picked[top + 8 : top + 16], 0.0), axis=0, keepdims=True
                )
                row_re = sky_re * last_re - sky_im * last_im
                row_im = sky_re * last_im + sky_im * last_re
            w = w_ref[k].astype(F32)
            both = jnp.concatenate([w * row_re, w * row_im], axis=0).astype(BF16)
            values_ref[k * 2 * cycles : (k + 1) * 2 * cycles, 0:width] = both
        hot_col = one_hot(col_ref[where].reshape(1, width), cols)
        sum_ref[...] += lax.dot_general(
            values_ref[:, 0:width],
            hot_col,
            (((1,), (1,)), ((), ())),
            preferred_element_type=F32,
        )

    add_chunk(streams[0], streams[1], pl.multiple_of(step * block, block), block)

    @pl.when(step == steps - 1)
    def _():
        if tail:
            add_chunk(streams[2], streams[3], steps * block, tail)
        share = cycles // shares
        for half in range(0, cols, LANES):
            size = min(cols - half, LANES)
            turn_ref[half // LANES, :, 0:size] = sum_ref[:, half : half + size]
        for t in range(cycles):
            top = t % share * 2 * orders
            for half in range(0, cols, LANES):
                size = min(cols - half, LANES)
                every = turn_ref[half // LANES, pl.ds(t, 2 * orders, stride=cycles), :]
                out_ref[t // share, top : top + 2 * orders, half : half + size] = every[:, 0:size]


def column_sums(wigner, sky_alm, beam, slot_col, slot_ell, cols, spans, shares):
    orders, cycles, slots = wigner.shape
    block = min(BLOCK, 2 ** (slots.bit_length() - 1))
    steps = slots // block
    tail = slots - steps * block
    rows = 2 * orders * cycles
    full = orders // 16 * 16
    table_rows = spans * 2 * full + 16 * (orders - full)
    whole = pl.BlockSpec(memory_space=pltpu.VMEM)

    def specs(width, at):
        return [
            pl.BlockSpec((orders, cycles, width), lambda i: (0, 0, at(i))),
            pl.BlockSpec((2, width), lambda i: (0, at(i))),
        ]

    in_specs = [whole, whole, whole] + specs(block, lambda i: i)
    operands = [slot_col, slot_ell, beam, wigner, sky_alm]
    if tail:
        at = slots // tail - 1
        in_specs += specs(tail, lambda i: at)
        operands += [wigner, sky_alm]
    out_shape = (shares, rows // shares, cols)
    return pl.pallas_call(
        functools.partial(sums_kernel, (cycles, orders, cols, spans, block, tail, steps, shares)),
        grid=(steps,),
        in_specs=in_specs,
        out_specs=pl.BlockSpec(out_shape, lambda i: (0, 0, 0)),
        scratch_shapes=[
            pltpu.VMEM((rows, cols), F32),
            pltpu.VMEM((rows, block), BF16),
            pltpu.VMEM((2, table_rows, TILE), BF16),
            pltpu.VMEM((table_rows, TILE + LANES), F32),
            pltpu.VMEM((-(-cols // LANES), rows, LANES), F32),
        ],
        out_shape=jax.ShapeDtypeStruct(out_shape, F32),
        compiler_params=pltpu.CompilerParams(
            dimension_semantics=("arbitrary",), vmem_limit_bytes=60 * 2**20
        ),
        name="column_sums",
    )(*operands)


def degree_width(degrees, ell_count, blk_count, cols):
    live = degrees * (degrees + 1) // 2 // (ell_count * blk_count)
    width = degrees - (ell_count - 1) * live // cols
    return min(degrees, -(-width // TILE) * TILE)


def on_device(wigner, sky_alm, beam_blm, slot_col, slot_ell, order_of_column):
    cycle_total = wigner.shape[0]
    order_count = wigner.shape[1]
    slot_count = wigner.shape[2]
    ell_count = lax.axis_size("ell")
    blk_count = lax.axis_size("blk")
    col_count = order_of_column.shape[0] // blk_count
    cycle_share = cycle_total // ell_count
    degree_count = beam_blm.shape[2]
    width = degree_width(degree_count, ell_count, blk_count, col_count)
    spans = width // TILE
    parts = column_sums(
        jnp.transpose(wigner, (1, 0, 2)),
        sky_alm,
        jnp.transpose(beam_blm, (1, 0, 2)),
        slot_col,
        slot_ell,
        col_count,
        spans,
        ell_count,
    )
    tables = phi_tables(order_of_column, 2 * degree_count)
    parts = lax.all_to_all(parts, "ell", split_axis=0, concat_axis=0, tiled=True)
    fields = to_psi(parts, blk_count, cycle_share, order_count)
    fields = lax.all_to_all(fields, "blk", split_axis=0, concat_axis=0, tiled=True)
    return to_phi(fields, tables, cycle_share)


def solution(mesh):
    return jax.shard_map(
        on_device,
        mesh=mesh,
        in_specs=(
            P(None, None, ("ell", "blk")),
            P(None, ("ell", "blk")),
            P(),
            P(("ell", "blk")),
            P(("ell", "blk")),
            P(),
        ),
        out_specs=P("ell", "blk", None),
        check_vma=False,
    )
```

```python
import functools
import math

import jax
import jax.numpy as jnp
import numpy as np
from jax import lax
from jax.experimental import pallas as pl
from jax.experimental.pallas import tpu as pltpu
from jax.sharding import PartitionSpec as P

NPSI = 32
LANES = 128
TILE = 256
BLOCK = 16384
PIECE = 1024
F32 = jnp.float32
BF16 = jnp.bfloat16


def psi_matrix(blks, cycles, orders):
    samples = NPSI // blks
    p = np.arange(NPSI).reshape(blks, 1, 1, samples, 1, 1, 1)
    cycle = np.arange(cycles)
    part = np.arange(2)
    k = np.arange(orders).reshape(1, 1, 1, 1, 1, 1, orders)
    same = cycle.reshape(1, -1, 1, 1, 1, 1, 1) == cycle.reshape(1, 1, 1, 1, -1, 1, 1)
    out_part = part.reshape(1, 1, 2, 1, 1, 1, 1)
    in_part = part.reshape(1, 1, 1, 1, 1, 2, 1)
    angle = 2.0 * np.pi * (k * p % NPSI) / NPSI
    turned = np.where(in_part == out_part, np.cos(angle), (out_part - in_part) * np.sin(angle))
    matrix = np.where(same, turned, 0.0).astype(np.float32)
    return matrix.reshape(blks * cycles * 2 * samples, cycles * orders * 2)


def psi_kernel(matrix_ref, *refs):
    total = refs[0][...]
    for part_ref in refs[1:-1]:
        total = total + part_ref[...]
    refs[-1][...] = jnp.dot(
        matrix_ref[...], total, precision=lax.Precision.HIGHEST, preferred_element_type=F32
    )


def to_psi(parts, blks, cycles, orders):
    matrix = psi_matrix(blks, cycles, orders)
    rows, cols = matrix.shape[0], parts[0].shape[1]
    out = pl.pallas_call(
        psi_kernel,
        out_shape=jax.ShapeDtypeStruct((rows, cols), F32),
        compiler_params=pltpu.CompilerParams(vmem_limit_bytes=16 * 2**20),
        name="psi",
    )(jnp.asarray(matrix), *parts)
    return out.reshape(blks, rows // blks, cols)


def halves(array):
    upper = lax.reduce_precision(array, exponent_bits=8, mantissa_bits=7)
    return upper.astype(BF16), (array - upper).astype(BF16)


def phi_tables(order_of_column, period):
    def waves(step, count):
        turns = jnp.arange(count, dtype=jnp.int32)[:, None] * step * order_of_column[None, :]
        angle = (turns % period).astype(F32) * (2.0 * math.pi / period)
        return jnp.cos(angle), jnp.sin(angle)

    fine_cos, fine_sin = waves(1, LANES)
    return waves(LANES, period // LANES) + halves(fine_cos) + halves(-fine_sin)


def phi_kernel(cycles, fields_ref, cos_ref, sin_ref, ch_ref, cl_ref, sh_ref, sl_ref, out_ref):
    blks, rows, cols = fields_ref.shape
    samples = rows // (2 * cycles)
    coarse = cos_ref.shape[0]

    def nt(left, right):
        return lax.dot_general(
            left, right, (((1,), (1,)), ((), ())), preferred_element_type=F32
        )

    def split(pieces):
        array = jnp.concatenate(pieces, axis=0)
        upper = array.astype(BF16)
        return upper, (array - upper.astype(F32)).astype(BF16)

    wide = None
    narrow = None
    for d in range(blks):
        where = slice(d * cols, (d + 1) * cols)
        cos, sin = cos_ref[:, where], sin_ref[:, where]
        left_re, left_im = [], []
        for t in range(cycles):
            for p in range(samples):
                at = t * 2 * samples + p
                re = fields_ref[d, at : at + 1, :]
                im = fields_ref[d, at + samples : at + samples + 1, :]
                left_re.append(re * cos - im * sin)
                left_im.append(re * sin + im * cos)
        for left, high_ref, low_ref in ((left_re, ch_ref, cl_ref), (left_im, sh_ref, sl_ref)):
            upper, lower = split(left)
            high, low = high_ref[:, where], low_ref[:, where]
            both = nt(upper, jnp.concatenate([high, low], axis=0))
            rest = nt(lower, high)
            wide = both if wide is None else wide + both
            narrow = rest if narrow is None else narrow + rest
    fine = high_ref.shape[0]
    result = wide[:, 0:fine] + (wide[:, fine:] + narrow)
    for t in range(cycles):
        for p in range(samples):
            for a in range(coarse):
                at = (t * samples + p) * coarse + a
                out_ref[t, p : p + 1, a * fine : (a + 1) * fine] = result[at : at + 1]


def to_phi(fields, tables, cycles):
    blks, rows, cols = fields.shape
    coarse, fine = tables[0].shape[0], tables[2].shape[0]
    samples = rows // (2 * cycles)
    return pl.pallas_call(
        functools.partial(phi_kernel, cycles),
        out_shape=jax.ShapeDtypeStruct((cycles, samples, coarse * fine), F32),
        compiler_params=pltpu.CompilerParams(vmem_limit_bytes=40 * 2**20),
        name="phi",
    )(fields, *tables)


def sums_kernel(shape, me_ref, col_ref, ell_ref, beam_ref, *refs):
    (cycles, orders, cols, spans, block, tail, steps, shares) = shape
    streams = refs[: -6 - shares]
    out_refs = refs[-6 - shares : -6]
    sum_ref, values_ref, table_ref, rows_ref, turn_ref, coef_ref = refs[-6:]
    step = pl.program_id(0)
    degrees = beam_ref.shape[2]
    full = orders // 16 * 16
    pair = 2 * full

    def lowest_degree():
        def fold(at, width, low):
            where = pl.ds(at, width)
            col = col_ref[where].reshape(1, width)
            ell = ell_ref[where].reshape(1, width).astype(F32)
            return jnp.minimum(low, jnp.min(jnp.where(col >= 0, ell, float(degrees))))

        low = float(degrees)
        low = lax.fori_loop(
            0, steps, lambda i, c: fold(pl.multiple_of(i * block, block), block, c), jnp.float32(low)
        )
        if tail:
            low = fold(steps * block, tail, low)
        return jnp.minimum(low.astype(jnp.int32), degrees - spans * TILE)

    @pl.when(step == 0)
    def _():
        sum_ref[...] = jnp.zeros_like(sum_ref)
        rows_ref[...] = jnp.zeros_like(rows_ref)
        base = lowest_degree()
        for k in range(orders):
            window = pltpu.roll(beam_ref[k], degrees - base, 1)
            for j in range(spans):
                for r in range(2):
                    row = j * pair + r * full + k
                    if k >= full:
                        row = spans * pair + (k - full) * 16 + 2 * j + r
                    rows_ref[row : row + 1, 0:TILE] = window[r : r + 1, j * TILE : (j + 1) * TILE]
        rows = rows_ref[:, 0:TILE]
        upper = rows.astype(BF16)
        table_ref[0] = upper
        table_ref[1] = (rows - upper.astype(F32)).astype(BF16)
        rows_ref[0:1, TILE:] = jnp.zeros((1, LANES), F32) + base.astype(F32)

    def one_hot(row, count):
        rows = lax.broadcasted_iota(jnp.int32, (count, row.shape[1]), 0).astype(F32).astype(BF16)
        match = row.astype(F32).astype(BF16) == rows
        return jnp.where(match, jnp.ones_like(rows), jnp.zeros_like(rows))

    def pick(sky_ref, first, at, width):
        index = ell_ref[pl.ds(at, width)].reshape(1, width) - base
        span = lax.shift_right_arithmetic(index, 8)
        hot_ell = one_hot(lax.bitwise_and(index, TILE - 1), TILE)
        picked = jnp.dot(table_ref[0], hot_ell, preferred_element_type=F32) + jnp.dot(
            table_ref[1], hot_ell, preferred_element_type=F32
        )
        beam_re = picked[0:full]
        beam_im = picked[full:pair]
        for j in range(1, spans):
            here = span == j
            beam_re = jnp.where(here, picked[j * pair : j * pair + full], beam_re)
            beam_im = jnp.where(here, picked[j * pair + full : (j + 1) * pair], beam_im)
        sky_re = sky_ref[0:1, first : first + width]
        sky_im = sky_ref[1:2, first : first + width]
        tiles = width // LANES
        start = first // LANES

        def keep(row, array):
            for i in range(tiles):
                coef_ref[start + i, row : row + array.shape[0], :] = array[
                    :, i * LANES : (i + 1) * LANES
                ]

        keep(0, sky_re * beam_re - sky_im * beam_im)
        keep(full, sky_re * beam_im + sky_im * beam_re)
        rows8 = lax.broadcasted_iota(jnp.int32, (8, width), 0)
        of_span = lax.shift_right_logical(rows8, 1)
        odd = lax.bitwise_and(rows8, 1) == 1
        signed = jnp.where(odd, sky_im, -sky_im)
        for k in range(full, orders):
            top = spans * pair + (k - full) * 16
            both = jnp.where(of_span == span, picked[top : top + 8], 0.0)
            if spans > 4:
                both = jnp.where(of_span + 4 == span, picked[top + 8 : top + 16], both)
            both = both + pltpu.roll(both, 4, 0)
            both = both + pltpu.roll(both, 2, 0)
            keep(pair + (k - full) * 8, both * sky_re + pltpu.roll(both, 1, 0) * signed)

    def spread(w_ref, first, width):
        for i in range(first // LANES, (first + width) // LANES):
            lanes = slice(i * LANES, (i + 1) * LANES)
            for k in range(orders):
                re_row, im_row = k, full + k
                if k >= full:
                    re_row = pair + (k - full) * 8
                    im_row = re_row + 1
                row_re = coef_ref[i, pl.ds(re_row, 8, stride=0), :]
                row_im = coef_ref[i, pl.ds(im_row, 8, stride=0), :]
                w = w_ref[k, :, lanes].astype(F32)
                for c in range(0, cycles, 8):
                    part = w[c : c + 8]
                    top = k * 2 * cycles + 2 * c
                    both = jnp.concatenate([part * row_re, part * row_im], axis=0).astype(BF16)
                    values_ref[top : top + 16, lanes] = both

    def add_chunk(w_ref, sky_ref, at, width):
        part = min(width, PIECE)
        for first in range(0, width, part):
            pick(sky_ref, first, at + first, part)
            spread(w_ref, first, part)
        hot_col = one_hot(col_ref[pl.ds(at, width)].reshape(1, width), cols)
        sum_ref[...] += lax.dot_general(
            values_ref[:, 0:width],
            hot_col,
            (((1,), (1,)), ((), ())),
            preferred_element_type=F32,
        )

    base = rows_ref[0:1, TILE : TILE + 1].astype(jnp.int32)
    add_chunk(streams[0], streams[1], pl.multiple_of(step * block, block), block)

    @pl.when(step == steps - 1)
    def _():
        if tail:
            add_chunk(streams[2], streams[3], steps * block, tail)
        share = cycles // shares
        for half in range(0, cols, LANES):
            size = min(cols - half, LANES)
            turn_ref[half // LANES, :, 0:size] = sum_ref[:, half : half + size]
        for d in range(shares):
            for i in range(share):
                t = lax.bitwise_xor(me_ref[0], d) * share + i
                start = t // 8 * 16 + t % 8
                for r in range(2):
                    top = (2 * i + r) * orders
                    rows = pl.ds(start + r * 8, orders, stride=2 * cycles)
                    for lane in range(0, cols, LANES):
                        size = min(cols - lane, LANES)
                        every = turn_ref[lane // LANES, rows, :]
                        out_refs[d][top : top + orders, lane : lane + size] = every[:, 0:size]


def column_sums(me, wigner, sky_alm, beam, slot_col, slot_ell, cols, spans, shares):
    orders, cycles, slots = wigner.shape
    block = min(BLOCK, 2 ** (slots.bit_length() - 1))
    steps = slots // block
    tail = slots - steps * block
    rows = 2 * orders * cycles
    full = orders // 16 * 16
    table_rows = spans * 2 * full + 16 * (orders - full)
    whole = pl.BlockSpec(memory_space=pltpu.VMEM)

    def specs(width, at):
        return [
            pl.BlockSpec((orders, cycles, width), lambda i: (0, 0, at(i))),
            pl.BlockSpec((2, width), lambda i: (0, at(i))),
        ]

    in_specs = [pl.BlockSpec(memory_space=pltpu.SMEM), whole, whole, whole] + specs(block, lambda i: i)
    operands = [me, slot_col, slot_ell, beam, wigner, sky_alm]
    if tail:
        at = slots // tail - 1
        in_specs += specs(tail, lambda i: at)
        operands += [wigner, sky_alm]
    out_shape = (rows // shares, cols)
    return pl.pallas_call(
        functools.partial(sums_kernel, (cycles, orders, cols, spans, block, tail, steps, shares)),
        grid=(steps,),
        in_specs=in_specs,
        out_specs=[pl.BlockSpec(out_shape, lambda i: (0, 0))] * shares,
        scratch_shapes=[
            pltpu.VMEM((rows, cols), F32),
            pltpu.VMEM((rows, block), BF16),
            pltpu.VMEM((2, table_rows, TILE), BF16),
            pltpu.VMEM((table_rows, TILE + LANES), F32),
            pltpu.VMEM((-(-cols // LANES), rows, LANES), F32),
            pltpu.VMEM((block // LANES, 2 * full + 8 * (orders - full), LANES), F32),
        ],
        out_shape=[jax.ShapeDtypeStruct(out_shape, F32)] * shares,
        compiler_params=pltpu.CompilerParams(
            dimension_semantics=("arbitrary",), vmem_limit_bytes=60 * 2**20
        ),
        name="column_sums",
    )(*operands)


def degree_width(degrees, ell_count, blk_count, cols):
    live = degrees * (degrees + 1) // 2 // (ell_count * blk_count)
    width = degrees - (ell_count - 1) * live // cols
    return min(degrees, -(-width // TILE) * TILE)


def on_device(wigner, sky_alm, beam_blm, slot_col, slot_ell, order_of_column):
    cycle_total = wigner.shape[0]
    order_count = wigner.shape[1]
    slot_count = wigner.shape[2]
    ell_count = lax.axis_size("ell")
    blk_count = lax.axis_size("blk")
    col_count = order_of_column.shape[0] // blk_count
    cycle_share = cycle_total // ell_count
    degree_count = beam_blm.shape[2]
    width = degree_width(degree_count, ell_count, blk_count, col_count)
    spans = width // TILE
    parts = column_sums(
        lax.axis_index("ell").reshape(1),
        jnp.transpose(wigner, (1, 0, 2)),
        sky_alm,
        jnp.transpose(beam_blm, (1, 0, 2)),
        slot_col,
        slot_ell,
        col_count,
        spans,
        ell_count,
    )
    tables = phi_tables(order_of_column, 2 * degree_count)
    parts = [
        part if d == 0 else lax.ppermute(part, "ell", [(i, i ^ d) for i in range(ell_count)])
        for d, part in enumerate(parts)
    ]
    fields = to_psi(parts, blk_count, cycle_share, order_count)
    fields = lax.all_to_all(fields, "blk", split_axis=0, concat_axis=0, tiled=True)
    return to_phi(fields, tables, cycle_share)


def solution(mesh):
    return jax.shard_map(
        on_device,
        mesh=mesh,
        in_specs=(
            P(None, None, ("ell", "blk")),
            P(None, ("ell", "blk")),
            P(),
            P(("ell", "blk")),
            P(("ell", "blk")),
            P(),
        ),
        out_specs=P("ell", "blk", None),
        check_vma=False,
    )
```

```python
import functools
import math

import jax
import jax.numpy as jnp
import numpy as np
from jax import lax
from jax.experimental import pallas as pl
from jax.experimental.pallas import tpu as pltpu
from jax.sharding import PartitionSpec as P

NPSI = 32
LANES = 128
TILE = 256
BLOCK = 16384
PIECE = 1024
F32 = jnp.float32
BF16 = jnp.bfloat16


def psi_matrix(blks, cycles, orders):
    samples = NPSI // blks
    p = np.arange(NPSI).reshape(blks, 1, 1, samples, 1, 1, 1)
    cycle = np.arange(cycles)
    part = np.arange(2)
    k = np.arange(orders).reshape(1, 1, 1, 1, 1, 1, orders)
    same = cycle.reshape(1, -1, 1, 1, 1, 1, 1) == cycle.reshape(1, 1, 1, 1, -1, 1, 1)
    out_part = part.reshape(1, 1, 2, 1, 1, 1, 1)
    in_part = part.reshape(1, 1, 1, 1, 1, 2, 1)
    angle = 2.0 * np.pi * (k * p % NPSI) / NPSI
    turned = np.where(in_part == out_part, np.cos(angle), (out_part - in_part) * np.sin(angle))
    matrix = np.where(same, turned, 0.0).astype(np.float32)
    return matrix.reshape(blks * cycles * 2 * samples, cycles * orders * 2)


def psi_kernel(matrix_ref, *refs):
    total = refs[0][...]
    for part_ref in refs[1:-1]:
        total = total + part_ref[...]
    refs[-1][...] = jnp.dot(
        matrix_ref[...], total, precision=lax.Precision.HIGHEST, preferred_element_type=F32
    )


def to_psi(parts, blks, cycles, orders):
    matrix = psi_matrix(blks, cycles, orders)
    rows, cols = matrix.shape[0], parts[0].shape[1]
    out = pl.pallas_call(
        psi_kernel,
        out_shape=jax.ShapeDtypeStruct((rows, cols), F32),
        compiler_params=pltpu.CompilerParams(vmem_limit_bytes=16 * 2**20),
        name="psi",
    )(jnp.asarray(matrix), *parts)
    return out.reshape(blks, rows // blks, cols)


def halves(array):
    upper = lax.reduce_precision(array, exponent_bits=8, mantissa_bits=7)
    return upper.astype(BF16), (array - upper).astype(BF16)


def phi_tables(order_of_column, period):
    def waves(step, count):
        turns = jnp.arange(count, dtype=jnp.int32)[:, None] * step * order_of_column[None, :]
        angle = (turns % period).astype(F32) * (2.0 * math.pi / period)
        return jnp.cos(angle), jnp.sin(angle)

    fine_cos, fine_sin = waves(1, LANES)
    return waves(LANES, period // LANES) + halves(fine_cos) + halves(-fine_sin)


def phi_kernel(cycles, fields_ref, cos_ref, sin_ref, ch_ref, cl_ref, sh_ref, sl_ref, out_ref):
    blks, rows, cols = fields_ref.shape
    samples = rows // (2 * cycles)
    coarse = cos_ref.shape[0]

    def nt(left, right):
        return lax.dot_general(
            left, right, (((1,), (1,)), ((), ())), preferred_element_type=F32
        )

    def split(pieces):
        array = jnp.concatenate(pieces, axis=0)
        upper = array.astype(BF16)
        return upper, (array - upper.astype(F32)).astype(BF16)

    wide = None
    narrow = None
    for d in range(blks):
        where = slice(d * cols, (d + 1) * cols)
        cos, sin = cos_ref[:, where], sin_ref[:, where]
        left_re, left_im = [], []
        for t in range(cycles):
            for p in range(samples):
                at = t * 2 * samples + p
                re = fields_ref[d, at : at + 1, :]
                im = fields_ref[d, at + samples : at + samples + 1, :]
                left_re.append(re * cos - im * sin)
                left_im.append(re * sin + im * cos)
        for left, high_ref, low_ref in ((left_re, ch_ref, cl_ref), (left_im, sh_ref, sl_ref)):
            upper, lower = split(left)
            high, low = high_ref[:, where], low_ref[:, where]
            both = nt(upper, jnp.concatenate([high, low], axis=0))
            rest = nt(lower, high)
            wide = both if wide is None else wide + both
            narrow = rest if narrow is None else narrow + rest
    fine = high_ref.shape[0]
    result = wide[:, 0:fine] + (wide[:, fine:] + narrow)
    for t in range(cycles):
        for p in range(samples):
            for a in range(coarse):
                at = (t * samples + p) * coarse + a
                out_ref[t, p : p + 1, a * fine : (a + 1) * fine] = result[at : at + 1]


def to_phi(fields, tables, cycles):
    blks, rows, cols = fields.shape
    coarse, fine = tables[0].shape[0], tables[2].shape[0]
    samples = rows // (2 * cycles)
    return pl.pallas_call(
        functools.partial(phi_kernel, cycles),
        out_shape=jax.ShapeDtypeStruct((cycles, samples, coarse * fine), F32),
        compiler_params=pltpu.CompilerParams(vmem_limit_bytes=40 * 2**20),
        name="phi",
    )(fields, *tables)


def sums_kernel(shape, me_ref, *refs):
    (cycles, orders, cols, spans, block, tail, steps, shares) = shape
    sources, wigner_ref, out_refs = refs[:4], refs[4], refs[5 : 5 + shares]
    (
        sum_ref,
        values_ref,
        table_ref,
        rows_ref,
        turn_ref,
        coef_ref,
        held_ref,
        last_ref,
        col_ref,
        ell_ref,
        beam_ref,
        sky_ref,
        sems,
    ) = refs[5 + shares :]
    degrees = beam_ref.shape[2]
    full = orders // 16 * 16
    pair = 2 * full

    def arrival(i):
        where = pl.ds(pl.multiple_of(i * block, block), block)
        slot = lax.rem(i, 2)
        return pltpu.make_async_copy(
            wigner_ref.at[:, :, where], held_ref.at[slot], sems.at[slot]
        )

    def last_arrival():
        where = pl.ds(steps * block, tail)
        return pltpu.make_async_copy(wigner_ref.at[:, :, where], last_ref, sems.at[2])

    small = [
        pltpu.make_async_copy(source, target, sems.at[3 + i])
        for i, (source, target) in enumerate(zip(sources, (col_ref, ell_ref, beam_ref, sky_ref)))
    ]
    for copy in small:
        copy.start()
    arrival(0).start()
    if tail:
        last_arrival().start()

    def lowest_degree():
        def fold(at, width, low):
            where = pl.ds(at, width)
            col = col_ref[where].reshape(1, width)
            ell = ell_ref[where].reshape(1, width).astype(F32)
            return jnp.minimum(low, jnp.min(jnp.where(col >= 0, ell, float(degrees))))

        low = float(degrees)
        low = lax.fori_loop(
            0, steps, lambda i, c: fold(pl.multiple_of(i * block, block), block, c), jnp.float32(low)
        )
        if tail:
            low = fold(steps * block, tail, low)
        return jnp.minimum(low.astype(jnp.int32), degrees - spans * TILE)

    sum_ref[...] = jnp.zeros_like(sum_ref)
    rows_ref[...] = jnp.zeros_like(rows_ref)
    for copy in small:
        copy.wait()
    base = lowest_degree()
    for k in range(orders):
        window = pltpu.roll(beam_ref[k], degrees - base, 1)
        for j in range(spans):
            for r in range(2):
                row = j * pair + r * full + k
                if k >= full:
                    row = spans * pair + (k - full) * 16 + 2 * j + r
                rows_ref[row : row + 1, 0:TILE] = window[r : r + 1, j * TILE : (j + 1) * TILE]
    rows = rows_ref[:, 0:TILE]
    upper = rows.astype(BF16)
    table_ref[0] = upper
    table_ref[1] = (rows - upper.astype(F32)).astype(BF16)
    rows_ref[0:1, TILE:] = jnp.zeros((1, LANES), F32) + base.astype(F32)

    def one_hot(row, count):
        rows = lax.broadcasted_iota(jnp.int32, (count, row.shape[1]), 0).astype(F32).astype(BF16)
        match = row.astype(F32).astype(BF16) == rows
        return jnp.where(match, jnp.ones_like(rows), jnp.zeros_like(rows))

    def pick(first, at, width):
        index = ell_ref[pl.ds(at, width)].reshape(1, width) - base
        span = lax.shift_right_arithmetic(index, 8)
        hot_ell = one_hot(lax.bitwise_and(index, TILE - 1), TILE)
        picked = jnp.dot(table_ref[0], hot_ell, preferred_element_type=F32) + jnp.dot(
            table_ref[1], hot_ell, preferred_element_type=F32
        )
        beam_re = picked[0:full]
        beam_im = picked[full:pair]
        for j in range(1, spans):
            here = span == j
            beam_re = jnp.where(here, picked[j * pair : j * pair + full], beam_re)
            beam_im = jnp.where(here, picked[j * pair + full : (j + 1) * pair], beam_im)
        sky_re = sky_ref[0:1, pl.ds(at, width)]
        sky_im = sky_ref[1:2, pl.ds(at, width)]
        tiles = width // LANES
        start = first // LANES

        def keep(row, array):
            for i in range(tiles):
                coef_ref[start + i, row : row + array.shape[0], :] = array[
                    :, i * LANES : (i + 1) * LANES
                ]

        keep(0, sky_re * beam_re - sky_im * beam_im)
        keep(full, sky_re * beam_im + sky_im * beam_re)
        rows8 = lax.broadcasted_iota(jnp.int32, (8, width), 0)
        of_span = lax.shift_right_logical(rows8, 1)
        odd = lax.bitwise_and(rows8, 1) == 1
        signed = jnp.where(odd, sky_im, -sky_im)
        for k in range(full, orders):
            top = spans * pair + (k - full) * 16
            both = jnp.where(of_span == span, picked[top : top + 8], 0.0)
            if spans > 4:
                both = jnp.where(of_span + 4 == span, picked[top + 8 : top + 16], both)
            both = both + pltpu.roll(both, 4, 0)
            both = both + pltpu.roll(both, 2, 0)
            keep(pair + (k - full) * 8, both * sky_re + pltpu.roll(both, 1, 0) * signed)

    def spread(w_ref, first, width):
        for i in range(first // LANES, (first + width) // LANES):
            lanes = slice(i * LANES, (i + 1) * LANES)
            for k in range(orders):
                re_row, im_row = k, full + k
                if k >= full:
                    re_row = pair + (k - full) * 8
                    im_row = re_row + 1
                row_re = coef_ref[i, pl.ds(re_row, 8, stride=0), :]
                row_im = coef_ref[i, pl.ds(im_row, 8, stride=0), :]
                w = w_ref[k, :, lanes].astype(F32)
                for c in range(0, cycles, 8):
                    part = w[c : c + 8]
                    top = k * 2 * cycles + 2 * c
                    both = jnp.concatenate([part * row_re, part * row_im], axis=0).astype(BF16)
                    values_ref[top : top + 16, lanes] = both

    def add_chunk(w_ref, at, width):
        part = min(width, PIECE)
        for first in range(0, width, part):
            pick(first, at + first, part)
            spread(w_ref, first, part)
        hot_col = one_hot(col_ref[pl.ds(at, width)].reshape(1, width), cols)
        sum_ref[...] += lax.dot_general(
            values_ref[:, 0:width],
            hot_col,
            (((1,), (1,)), ((), ())),
            preferred_element_type=F32,
        )

    base = rows_ref[0:1, TILE : TILE + 1].astype(jnp.int32)

    def body(i, carry):
        arrival(i).wait()

        @pl.when(i + 1 < steps)
        def _():
            arrival(i + 1).start()

        add_chunk(held_ref.at[lax.rem(i, 2)], pl.multiple_of(i * block, block), block)
        return carry

    lax.fori_loop(0, steps, body, 0)
    if tail:
        last_arrival().wait()
        add_chunk(last_ref, steps * block, tail)
    share = cycles // shares
    for half in range(0, cols, LANES):
        size = min(cols - half, LANES)
        turn_ref[half // LANES, :, 0:size] = sum_ref[:, half : half + size]
    for d in range(shares):
        for i in range(share):
            t = lax.bitwise_xor(me_ref[0], d) * share + i
            start = t // 8 * 16 + t % 8
            for r in range(2):
                top = (2 * i + r) * orders
                rows = pl.ds(start + r * 8, orders, stride=2 * cycles)
                for lane in range(0, cols, LANES):
                    size = min(cols - lane, LANES)
                    every = turn_ref[lane // LANES, rows, :]
                    out_refs[d][top : top + orders, lane : lane + size] = every[:, 0:size]


def column_sums(me, wigner, sky_alm, beam, slot_col, slot_ell, cols, spans, shares):
    orders, cycles, slots = wigner.shape
    block = min(BLOCK, 2 ** (slots.bit_length() - 1))
    steps = slots // block
    tail = slots - steps * block
    rows = 2 * orders * cycles
    full = orders // 16 * 16
    table_rows = spans * 2 * full + 16 * (orders - full)
    whole = pl.BlockSpec(memory_space=pltpu.VMEM)

    out_shape = (rows // shares, cols)
    return pl.pallas_call(
        functools.partial(sums_kernel, (cycles, orders, cols, spans, block, tail, steps, shares)),
        in_specs=[pl.BlockSpec(memory_space=pltpu.SMEM)]
        + [pl.BlockSpec(memory_space=pltpu.HBM)] * 5,
        out_specs=[whole] * shares,
        scratch_shapes=[
            pltpu.VMEM((rows, cols), F32),
            pltpu.VMEM((rows, block), BF16),
            pltpu.VMEM((2, table_rows, TILE), BF16),
            pltpu.VMEM((table_rows, TILE + LANES), F32),
            pltpu.VMEM((-(-cols // LANES), rows, LANES), F32),
            pltpu.VMEM((block // LANES, 2 * full + 8 * (orders - full), LANES), F32),
            pltpu.VMEM((2, orders, cycles, block), BF16),
            pltpu.VMEM((orders, cycles, max(tail, LANES)), BF16),
            pltpu.VMEM(slot_col.shape, slot_col.dtype),
            pltpu.VMEM(slot_ell.shape, slot_ell.dtype),
            pltpu.VMEM(beam.shape, beam.dtype),
            pltpu.VMEM(sky_alm.shape, sky_alm.dtype),
            pltpu.SemaphoreType.DMA((7,)),
        ],
        out_shape=[jax.ShapeDtypeStruct(out_shape, F32)] * shares,
        compiler_params=pltpu.CompilerParams(vmem_limit_bytes=54784 * 2**10),
        name="column_sums",
    )(me, slot_col, slot_ell, beam, sky_alm, wigner)


def degree_width(degrees, ell_count, blk_count, cols):
    live = degrees * (degrees + 1) // 2 // (ell_count * blk_count)
    width = degrees - (ell_count - 1) * live // cols
    return min(degrees, -(-width // TILE) * TILE)


def on_device(wigner, sky_alm, beam_blm, slot_col, slot_ell, order_of_column):
    cycle_total = wigner.shape[0]
    order_count = wigner.shape[1]
    slot_count = wigner.shape[2]
    ell_count = lax.axis_size("ell")
    blk_count = lax.axis_size("blk")
    col_count = order_of_column.shape[0] // blk_count
    cycle_share = cycle_total // ell_count
    degree_count = beam_blm.shape[2]
    width = degree_width(degree_count, ell_count, blk_count, col_count)
    spans = width // TILE
    parts = column_sums(
        lax.axis_index("ell").reshape(1),
        jnp.transpose(wigner, (1, 0, 2)),
        sky_alm,
        jnp.transpose(beam_blm, (1, 0, 2)),
        slot_col,
        slot_ell,
        col_count,
        spans,
        ell_count,
    )
    tables = phi_tables(order_of_column, 2 * degree_count)
    parts = [
        part if d == 0 else lax.ppermute(part, "ell", [(i, i ^ d) for i in range(ell_count)])
        for d, part in enumerate(parts)
    ]
    fields = to_psi(parts, blk_count, cycle_share, order_count)
    fields = lax.all_to_all(fields, "blk", split_axis=0, concat_axis=0, tiled=True)
    return to_phi(fields, tables, cycle_share)


def solution(mesh):
    return jax.shard_map(
        on_device,
        mesh=mesh,
        in_specs=(
            P(None, None, ("ell", "blk")),
            P(None, ("ell", "blk")),
            P(),
            P(("ell", "blk")),
            P(("ell", "blk")),
            P(),
        ),
        out_specs=P("ell", "blk", None),
        check_vma=False,
    )
```

```python
import functools
import math

import jax
import jax.numpy as jnp
import numpy as np
from jax import lax
from jax.experimental import pallas as pl
from jax.experimental.pallas import tpu as pltpu
from jax.sharding import PartitionSpec as P

NPSI = 32
LANES = 128
TILE = 256
BLOCK = 16384
PIECE = 1024
F32 = jnp.float32
BF16 = jnp.bfloat16


def psi_matrix(blks, cycles, orders):
    samples = NPSI // blks
    p = np.arange(NPSI).reshape(blks, 1, 1, samples, 1, 1, 1)
    cycle = np.arange(cycles)
    part = np.arange(2)
    k = np.arange(orders).reshape(1, 1, 1, 1, 1, 1, orders)
    same = cycle.reshape(1, -1, 1, 1, 1, 1, 1) == cycle.reshape(1, 1, 1, 1, -1, 1, 1)
    out_part = part.reshape(1, 1, 2, 1, 1, 1, 1)
    in_part = part.reshape(1, 1, 1, 1, 1, 2, 1)
    angle = 2.0 * np.pi * (k * p % NPSI) / NPSI
    turned = np.where(in_part == out_part, np.cos(angle), (out_part - in_part) * np.sin(angle))
    matrix = np.where(same, turned, 0.0).astype(np.float32)
    return matrix.reshape(blks * cycles * 2 * samples, cycles * orders * 2)


def psi_kernel(high_ref, low_ref, *refs):
    total = refs[0][...]
    for part_ref in refs[1:-1]:
        total = total + part_ref[...]
    upper = total.astype(BF16)
    lower = (total - upper.astype(F32)).astype(BF16)

    def product(left, right):
        return jnp.dot(left, right, preferred_element_type=F32)

    high = high_ref[...]
    refs[-1][...] = product(high, upper) + (product(high, lower) + product(low_ref[...], upper))


def to_psi(parts, blks, cycles, orders):
    matrix = psi_matrix(blks, cycles, orders)
    upper = matrix.astype(BF16)
    lower = (matrix - upper.astype(np.float32)).astype(BF16)
    rows, cols = matrix.shape[0], parts[0].shape[1]
    out = pl.pallas_call(
        psi_kernel,
        out_shape=jax.ShapeDtypeStruct((rows, cols), F32),
        compiler_params=pltpu.CompilerParams(vmem_limit_bytes=16 * 2**20),
        name="psi",
    )(jnp.asarray(upper), jnp.asarray(lower), *parts)
    return out.reshape(blks, rows // blks, cols)


def halves(array):
    upper = lax.reduce_precision(array, exponent_bits=8, mantissa_bits=7)
    return upper.astype(BF16), (array - upper).astype(BF16)


def phi_tables(order_of_column, period):
    def waves(step, count):
        turns = jnp.arange(count, dtype=jnp.int32)[:, None] * step * order_of_column[None, :]
        angle = (turns % period).astype(F32) * (2.0 * math.pi / period)
        return jnp.cos(angle), jnp.sin(angle)

    fine_cos, fine_sin = waves(1, LANES)
    return waves(LANES, period // LANES) + halves(fine_cos) + halves(-fine_sin)


def phi_kernel(cycles, fields_ref, cos_ref, sin_ref, ch_ref, cl_ref, sh_ref, sl_ref, out_ref):
    blks, rows, cols = fields_ref.shape
    samples = rows // (2 * cycles)
    coarse = cos_ref.shape[0]

    def nt(left, right):
        return lax.dot_general(
            left, right, (((1,), (1,)), ((), ())), preferred_element_type=F32
        )

    def split(pieces):
        array = jnp.concatenate(pieces, axis=0)
        upper = array.astype(BF16)
        return upper, (array - upper.astype(F32)).astype(BF16)

    wide = None
    narrow = None
    for d in range(blks):
        where = slice(d * cols, (d + 1) * cols)
        cos, sin = cos_ref[:, where], sin_ref[:, where]
        left_re, left_im = [], []
        for t in range(cycles):
            for p in range(samples):
                at = t * 2 * samples + p
                re = fields_ref[d, at : at + 1, :]
                im = fields_ref[d, at + samples : at + samples + 1, :]
                left_re.append(re * cos - im * sin)
                left_im.append(re * sin + im * cos)
        for left, high_ref, low_ref in ((left_re, ch_ref, cl_ref), (left_im, sh_ref, sl_ref)):
            upper, lower = split(left)
            high, low = high_ref[:, where], low_ref[:, where]
            both = nt(upper, jnp.concatenate([high, low], axis=0))
            rest = nt(lower, high)
            wide = both if wide is None else wide + both
            narrow = rest if narrow is None else narrow + rest
    fine = high_ref.shape[0]
    result = wide[:, 0:fine] + (wide[:, fine:] + narrow)
    for t in range(cycles):
        for p in range(samples):
            for a in range(coarse):
                at = (t * samples + p) * coarse + a
                out_ref[t, p : p + 1, a * fine : (a + 1) * fine] = result[at : at + 1]


def to_phi(fields, tables, cycles):
    blks, rows, cols = fields.shape
    coarse, fine = tables[0].shape[0], tables[2].shape[0]
    samples = rows // (2 * cycles)
    return pl.pallas_call(
        functools.partial(phi_kernel, cycles),
        out_shape=jax.ShapeDtypeStruct((cycles, samples, coarse * fine), F32),
        compiler_params=pltpu.CompilerParams(vmem_limit_bytes=40 * 2**20),
        name="phi",
    )(fields, *tables)


def sums_kernel(shape, me_ref, *refs):
    (cycles, orders, cols, spans, block, tail, steps, shares) = shape
    sources, wigner_ref, out_refs = refs[:4], refs[4], refs[5 : 5 + shares]
    (
        sum_ref,
        values_ref,
        table_ref,
        rows_ref,
        turn_ref,
        coef_ref,
        held_ref,
        last_ref,
        col_ref,
        ell_ref,
        beam_ref,
        sky_ref,
        sems,
    ) = refs[5 + shares :]
    degrees = beam_ref.shape[2]
    full = orders // 16 * 16
    pair = 2 * full

    def arrival(i):
        where = pl.ds(pl.multiple_of(i * block, block), block)
        slot = lax.rem(i, 2)
        return pltpu.make_async_copy(
            wigner_ref.at[:, :, where], held_ref.at[slot], sems.at[slot]
        )

    def last_arrival():
        where = pl.ds(steps * block, tail)
        return pltpu.make_async_copy(wigner_ref.at[:, :, where], last_ref, sems.at[2])

    small = [
        pltpu.make_async_copy(source, target, sems.at[3 + i])
        for i, (source, target) in enumerate(zip(sources, (col_ref, ell_ref, beam_ref, sky_ref)))
    ]
    for copy in small:
        copy.start()
    arrival(0).start()
    if tail:
        last_arrival().start()

    def lowest_degree():
        def fold(at, width, low):
            where = pl.ds(at, width)
            shape = (width // LANES, LANES)
            col = col_ref[where].reshape(shape)
            ell = ell_ref[where].reshape(shape).astype(F32)
            return jnp.minimum(low, jnp.min(jnp.where(col >= 0, ell, float(degrees))))

        low = float(degrees)
        low = lax.fori_loop(
            0, steps, lambda i, c: fold(pl.multiple_of(i * block, block), block, c), jnp.float32(low)
        )
        if tail:
            low = fold(steps * block, tail, low)
        return jnp.minimum(low.astype(jnp.int32), degrees - spans * TILE)

    sum_ref[...] = jnp.zeros_like(sum_ref)
    rows_ref[...] = jnp.zeros_like(rows_ref)
    for copy in small:
        copy.wait()
    base = lowest_degree()
    for k in range(orders):
        window = pltpu.roll(beam_ref[k], degrees - base, 1)
        for j in range(spans):
            for r in range(2):
                row = j * pair + r * full + k
                if k >= full:
                    row = spans * pair + (k - full) * 16 + 2 * j + r
                rows_ref[row : row + 1, 0:TILE] = window[r : r + 1, j * TILE : (j + 1) * TILE]
    rows = rows_ref[:, 0:TILE]
    upper = rows.astype(BF16)
    table_ref[0] = upper
    table_ref[1] = (rows - upper.astype(F32)).astype(BF16)
    rows_ref[0:1, TILE:] = jnp.zeros((1, LANES), F32) + base.astype(F32)

    def one_hot(row, count):
        rows = lax.broadcasted_iota(jnp.int32, (count, row.shape[1]), 0).astype(F32).astype(BF16)
        match = row.astype(F32).astype(BF16) == rows
        return jnp.where(match, jnp.ones_like(rows), jnp.zeros_like(rows))

    def pick(first, at, width):
        index = ell_ref[pl.ds(at, width)].reshape(1, width) - base
        span = lax.shift_right_arithmetic(index, 8)
        hot_ell = one_hot(lax.bitwise_and(index, TILE - 1), TILE)
        picked = jnp.dot(table_ref[0], hot_ell, preferred_element_type=F32) + jnp.dot(
            table_ref[1], hot_ell, preferred_element_type=F32
        )
        beam_re = picked[0:full]
        beam_im = picked[full:pair]
        for j in range(1, spans):
            here = span == j
            beam_re = jnp.where(here, picked[j * pair : j * pair + full], beam_re)
            beam_im = jnp.where(here, picked[j * pair + full : (j + 1) * pair], beam_im)
        sky_re = sky_ref[0:1, pl.ds(at, width)]
        sky_im = sky_ref[1:2, pl.ds(at, width)]
        tiles = width // LANES
        start = first // LANES

        def keep(row, array):
            for i in range(tiles):
                coef_ref[start + i, row : row + array.shape[0], :] = array[
                    :, i * LANES : (i + 1) * LANES
                ]

        keep(0, sky_re * beam_re - sky_im * beam_im)
        keep(full, sky_re * beam_im + sky_im * beam_re)
        rows8 = lax.broadcasted_iota(jnp.int32, (8, width), 0)
        of_span = lax.shift_right_logical(rows8, 1)
        odd = lax.bitwise_and(rows8, 1) == 1
        signed = jnp.where(odd, sky_im, -sky_im)
        for k in range(full, orders):
            top = spans * pair + (k - full) * 16
            both = jnp.where(of_span == span, picked[top : top + 8], 0.0)
            if spans > 4:
                both = jnp.where(of_span + 4 == span, picked[top + 8 : top + 16], both)
            both = both + pltpu.roll(both, 4, 0)
            both = both + pltpu.roll(both, 2, 0)
            keep(pair + (k - full) * 8, both * sky_re + pltpu.roll(both, 1, 0) * signed)

    def spread(w_ref, first, width):
        for i in range(first // LANES, (first + width) // LANES):
            lanes = slice(i * LANES, (i + 1) * LANES)
            for k in range(orders):
                re_row, im_row = k, full + k
                if k >= full:
                    re_row = pair + (k - full) * 8
                    im_row = re_row + 1
                row_re = coef_ref[i, pl.ds(re_row, 8, stride=0), :]
                row_im = coef_ref[i, pl.ds(im_row, 8, stride=0), :]
                w = w_ref[k, :, lanes].astype(F32)
                for c in range(0, cycles, 8):
                    part = w[c : c + 8]
                    top = k * 2 * cycles + 2 * c
                    both = jnp.concatenate([part * row_re, part * row_im], axis=0).astype(BF16)
                    values_ref[top : top + 16, lanes] = both

    def add_chunk(w_ref, at, width):
        part = min(width, PIECE)
        for first in range(0, width, part):
            pick(first, at + first, part)
            spread(w_ref, first, part)
        hot_col = one_hot(col_ref[pl.ds(at, width)].reshape(1, width), cols)
        sum_ref[...] += lax.dot_general(
            values_ref[:, 0:width],
            hot_col,
            (((1,), (1,)), ((), ())),
            preferred_element_type=F32,
        )

    base = rows_ref[0:1, TILE : TILE + 1].astype(jnp.int32)

    def body(i, carry):
        arrival(i).wait()

        @pl.when(i + 1 < steps)
        def _():
            arrival(i + 1).start()

        add_chunk(held_ref.at[lax.rem(i, 2)], pl.multiple_of(i * block, block), block)
        return carry

    lax.fori_loop(0, steps, body, 0)
    if tail:
        last_arrival().wait()
        add_chunk(last_ref, steps * block, tail)
    share = cycles // shares
    for half in range(0, cols, LANES):
        size = min(cols - half, LANES)
        turn_ref[half // LANES, :, 0:size] = sum_ref[:, half : half + size]
    for d in range(shares):
        for i in range(share):
            t = lax.bitwise_xor(me_ref[0], d) * share + i
            start = t // 8 * 16 + t % 8
            for r in range(2):
                top = (2 * i + r) * orders
                rows = pl.ds(start + r * 8, orders, stride=2 * cycles)
                for lane in range(0, cols, LANES):
                    size = min(cols - lane, LANES)
                    every = turn_ref[lane // LANES, rows, :]
                    out_refs[d][top : top + orders, lane : lane + size] = every[:, 0:size]


def column_sums(me, wigner, sky_alm, beam, slot_col, slot_ell, cols, spans, shares):
    orders, cycles, slots = wigner.shape
    block = min(BLOCK, 2 ** (slots.bit_length() - 1))
    steps = slots // block
    tail = slots - steps * block
    rows = 2 * orders * cycles
    full = orders // 16 * 16
    table_rows = spans * 2 * full + 16 * (orders - full)
    whole = pl.BlockSpec(memory_space=pltpu.VMEM)

    out_shape = (rows // shares, cols)
    return pl.pallas_call(
        functools.partial(sums_kernel, (cycles, orders, cols, spans, block, tail, steps, shares)),
        in_specs=[pl.BlockSpec(memory_space=pltpu.SMEM)]
        + [pl.BlockSpec(memory_space=pltpu.HBM)] * 5,
        out_specs=[whole] * shares,
        scratch_shapes=[
            pltpu.VMEM((rows, cols), F32),
            pltpu.VMEM((rows, block), BF16),
            pltpu.VMEM((2, table_rows, TILE), BF16),
            pltpu.VMEM((table_rows, TILE + LANES), F32),
            pltpu.VMEM((-(-cols // LANES), rows, LANES), F32),
            pltpu.VMEM((block // LANES, 2 * full + 8 * (orders - full), LANES), F32),
            pltpu.VMEM((2, orders, cycles, block), BF16),
            pltpu.VMEM((orders, cycles, max(tail, LANES)), BF16),
            pltpu.VMEM(slot_col.shape, slot_col.dtype),
            pltpu.VMEM(slot_ell.shape, slot_ell.dtype),
            pltpu.VMEM(beam.shape, beam.dtype),
            pltpu.VMEM(sky_alm.shape, sky_alm.dtype),
            pltpu.SemaphoreType.DMA((7,)),
        ],
        out_shape=[jax.ShapeDtypeStruct(out_shape, F32)] * shares,
        compiler_params=pltpu.CompilerParams(vmem_limit_bytes=54784 * 2**10),
        name="column_sums",
    )(me, slot_col, slot_ell, beam, sky_alm, wigner)


def degree_width(degrees, ell_count, blk_count, cols):
    live = degrees * (degrees + 1) // 2 // (ell_count * blk_count)
    width = degrees - (ell_count - 1) * live // cols
    return min(degrees, -(-width // TILE) * TILE)


def on_device(wigner, sky_alm, beam_blm, slot_col, slot_ell, order_of_column):
    cycle_total = wigner.shape[0]
    order_count = wigner.shape[1]
    slot_count = wigner.shape[2]
    ell_count = lax.axis_size("ell")
    blk_count = lax.axis_size("blk")
    col_count = order_of_column.shape[0] // blk_count
    cycle_share = cycle_total // ell_count
    degree_count = beam_blm.shape[2]
    width = degree_width(degree_count, ell_count, blk_count, col_count)
    spans = width // TILE
    parts = column_sums(
        lax.axis_index("ell").reshape(1),
        jnp.transpose(wigner, (1, 0, 2)),
        sky_alm,
        jnp.transpose(beam_blm, (1, 0, 2)),
        slot_col,
        slot_ell,
        col_count,
        spans,
        ell_count,
    )
    parts = [
        part if d == 0 else lax.ppermute(part, "ell", [(i, i ^ d) for i in range(ell_count)])
        for d, part in enumerate(parts)
    ]
    fields = to_psi(parts, blk_count, cycle_share, order_count)
    fields, order_of_column = lax.optimization_barrier((fields, order_of_column))
    tables = phi_tables(order_of_column, 2 * degree_count)
    fields = lax.all_to_all(fields, "blk", split_axis=0, concat_axis=0, tiled=True)
    return to_phi(fields, tables, cycle_share)


def solution(mesh):
    return jax.shard_map(
        on_device,
        mesh=mesh,
        in_specs=(
            P(None, None, ("ell", "blk")),
            P(None, ("ell", "blk")),
            P(),
            P(("ell", "blk")),
            P(("ell", "blk")),
            P(),
        ),
        out_specs=P("ell", "blk", None),
        check_vma=False,
    )
```
